32 devices in a mesh: img: 4 (over z), seq: 8 (over y, x, core).
Axes of the slice: x: 2, y: 2, z: 4, core: 2. Of those that a mesh axis runs over, the one named last changes fastest.
Arguments:
- queries: bfloat16 [4, 512, 4096], P('img', 'seq')
- keys: bfloat16 [4, 512, 4096], P('img', 'seq')
- values: bfloat16 [4, 512, 4096], P('img', 'seq'), may hold values from -6 to 6
- counts: int32 [4], replicated, may hold values from 1 to 128
- offsets: int32 [4, 4], replicated, may hold values from 0 to 480, as said below
- text: bfloat16 [512, 8192], P('img', 'seq'), may hold values from -6 to 6
- w_proj: bfloat16 [4096, 8192], P(None, 'seq'), may hold values from -0.09375 to 0.09375
- gain: float32 [8192], P('seq'), may hold values from 0.5 to 1.5
Outputs:
- normed: bfloat16 [512, 8192], P('img', 'seq')
The draws below stay inside these ranges and needn't reach their ends.
Inputs may be any that keep to these rules, and one draw needn't show every extreme that they name: Each image keeps its first counts pooled tokens. `offsets`: each entry is a multiple of 32. Position p belongs to sequence block p // 128. The 4 blocks of one image start in 4 different sequence blocks, and each sequence block receives exactly one block of every image, so the blocks cover the language sequence once.
All inputs are finite; a program needn't handle non-finite values.
Results may differ from the reference program's by a relative error of at most 0.0043.
Values may be sent and summed in bfloat16 or wider, within the bound.
No kernel may reach another device: no remote copies, remote signals or barrier semaphores. Data moves between devices by JAX's collectives and lax.ppermute only.
A program may use at most 64 MiB of HBM per device.

```python
import jax
import jax.numpy as jnp
from jax import lax

HD = 128
LD = 8192
POOL = 4
IMAGES = 4
PATCHES = 512
AW = 4096
NPOOL = 128
LSEQ = 512
N_IMG = 4


def query_key_pair(key):
    first_key = jax.random.fold_in(key, 71)
    second_key = jax.random.fold_in(key, 73)
    queries = jax.random.normal(first_key, (IMAGES, PATCHES, AW), jnp.float32)
    keys = jax.random.normal(second_key, (IMAGES, PATCHES, AW), jnp.float32)
    return (queries, keys)


def draw_queries(key, part):
    return query_key_pair(key)[0].astype(jnp.bfloat16)


def draw_keys(key, part):
    return query_key_pair(key)[1].astype(jnp.bfloat16)


def draw_offsets(key, part):
    owners = N_IMG
    block_rows = PATCHES // POOL // N_IMG
    seq_block = PATCHES // POOL
    image_ids = jnp.arange(owners, dtype=jnp.int32)
    owner_table = jax.vmap(lambda image: jax.random.permutation(jax.random.fold_in(key, image), owners))(image_ids)
    slot_perms = jax.vmap(lambda owner: jax.random.permutation(jax.random.fold_in(key, owner + 100000), owners))(image_ids)
    slot_table = slot_perms[owner_table, image_ids[:, None]]
    return (owner_table * seq_block + slot_table * block_rows).astype(jnp.int32)


def set_ends(values, stream_key, least, largest):
    shape = values.shape
    spot = [jax.random.randint(jax.random.fold_in(stream_key, axis), (), 0, shape[axis]) for axis in range(len(shape))]
    values = values.at[tuple(spot)].set(least)
    longest = shape.index(max(shape))
    spot[longest] = (spot[longest] + 1) % shape[longest]
    return values.at[tuple(spot)].set(largest)


def block_levels(key, extent, cuts, smallest, top_value):
    def one(dim, parts):
        steps = jax.random.uniform(jax.random.fold_in(jax.random.fold_in(key, 6), dim), (parts,), jnp.float32, smallest / len(cuts), top_value / len(cuts))
        return jnp.repeat(jnp.exp(steps), extent[dim] // parts).reshape((-1,) + (1,) * (len(extent) - dim - 1))

    level = one(*cuts[0])
    for cut in cuts[1:]:
        level = level * one(*cut)
    return level


def normal_values(stream_key, dims, scale, reach, pieces=(), kind=jnp.bfloat16):
    values = scale * jax.random.normal(stream_key, dims, jnp.float32)
    if pieces:
        values = values * block_levels(stream_key, dims, pieces, -0.22, 0.18)
    return jnp.clip(values, -reach, reach).astype(kind)


def setup_inputs(seed: int = 0) -> dict:
    key_of = jax.random.split(jax.random.key(seed), 9)
    queries = draw_queries(jax.random.fold_in(key_of[8], 71), 0)
    keys = draw_keys(jax.random.fold_in(key_of[8], 71), 0)
    values = normal_values(key_of[2], (IMAGES, PATCHES, AW), 1.0, 6.0, ((0, 4), (1, 8)))
    counts = set_ends(jax.random.randint(key_of[3], (IMAGES,), 1, NPOOL + 1), jax.random.fold_in(key_of[3], 1), 1, NPOOL).astype(jnp.int32)
    offsets = draw_offsets(jax.random.fold_in(key_of[8], 71), 0)
    text = normal_values(key_of[5], (LSEQ, LD), 1.0, 6.0, ((0, 4), (1, 8)))
    w_proj = normal_values(key_of[6], (AW, LD), AW ** -0.5, 0.09375, ((1, 8),))
    gain = jnp.clip(1.0 + 0.1 * jax.random.normal(key_of[7], (LD,), jnp.float32), 0.5, 1.5)
    return dict(queries=queries, keys=keys, values=values, counts=counts, offsets=offsets, text=text, w_proj=w_proj, gain=gain)


EPSILON = 1e-05

def attend(query, keys, values):
    patches, feature_dim = query.shape
    head_count = feature_dim // HD
    query_block = min(512, patches)
    query_split = query.astype(jnp.float32).reshape(patches // query_block, query_block, head_count, HD)
    keys_split = keys.astype(jnp.float32).reshape(patches, head_count, HD)
    values_split = values.astype(jnp.float32).reshape(patches, head_count, HD)
    score_scale = HD ** (-0.5)

    def one_block(query_rows):
        scores = jnp.einsum('qhd,khd->hqk', query_rows, keys_split) * score_scale
        row_peak = lax.optimization_barrier(jnp.max(scores, axis=2, keepdims=True))
        exponent = jnp.exp(scores - row_peak)
        weights = (exponent / lax.optimization_barrier(jnp.sum(exponent, axis=2, keepdims=True))).astype(jnp.bfloat16)
        weights = lax.optimization_barrier(weights).astype(jnp.float32)
        return jnp.einsum('hqk,khd->qhd', weights, values_split).reshape(query_block, head_count * HD)
    return lax.map(one_block, query_split).reshape(patches, feature_dim)

def per_image(triple):
    attended = attend(triple[0], triple[1], triple[2])
    patches, feature_dim = attended.shape
    summed = lax.optimization_barrier(jnp.sum(attended.reshape(patches // POOL, POOL, feature_dim), axis=1))
    return (summed / POOL).astype(jnp.bfloat16)

def reference(queries, keys, values, counts, offsets, text, w_proj, gain):
    pooled = lax.map(per_image, (queries, keys, values))
    pool_count = pooled.shape[1]
    block_rows = pool_count // N_IMG
    total_len = pool_count * N_IMG
    positions = (offsets[:, :, None] + jnp.arange(block_rows, dtype=jnp.int32)[None, None, :]).reshape(-1).astype(jnp.int32)
    visual = jnp.zeros((total_len, AW), jnp.bfloat16).at[positions].set(pooled.reshape(-1, AW))
    kept_rows = (jnp.arange(pool_count, dtype=jnp.int32)[None, :] < counts[:, None]).reshape(-1)
    live_rows = jnp.zeros((total_len,), bool).at[positions].set(kept_rows)
    projected = jnp.dot(visual, w_proj, preferred_element_type=jnp.float32)
    hidden = jnp.where(live_rows[:, None], projected, text.astype(jnp.float32))
    square_sum = lax.optimization_barrier(jnp.sum(hidden * hidden, axis=1, keepdims=True))
    normed = hidden * lax.rsqrt(square_sum / LD + EPSILON) * gain.astype(jnp.float32)[None, :]
    return normed.astype(jnp.bfloat16)
```

```python
import functools
import math

import jax
import jax.numpy as jnp
from jax import lax
from jax.experimental import pallas as pl
from jax.experimental.pallas import tpu as pltpu
from jax.sharding import PartitionSpec as P

HD = 128
POOL = 4
EPSILON = 1e-05
BF16 = jnp.bfloat16
F32 = jnp.float32


def vmem():
    return pl.BlockSpec(memory_space=pltpu.VMEM)


def smem():
    return pl.BlockSpec(memory_space=pltpu.SMEM)


def anywhere():
    return pl.BlockSpec(memory_space=pl.ANY)


def chunk_heads(heads):
    tail = max(1, heads // 4)
    return [heads - tail, tail] if heads > tail else [heads]


def pack_body(columns, *refs, pieces, first, width):
    q_ref, k_ref, v_ref = refs[:3]
    outs, sems = refs[3:-1], refs[-1]
    copies = []
    for p in range(pieces):
        start = pl.multiple_of(columns[p] + first, HD)
        for t, src in enumerate((q_ref, k_ref, v_ref)):
            copies.append(
                pltpu.make_async_copy(
                    src.at[0, :, pl.ds(start, width)], outs[p].at[t], sems.at[p, t]
                )
            )
    for c in copies:
        c.start()
    for c in copies:
        c.wait()


def pack(columns, queries, keys, values, pieces, first, width):
    rows = queries.shape[1]
    return pl.pallas_call(
        functools.partial(pack_body, pieces=pieces, first=first, width=width),
        out_shape=[jax.ShapeDtypeStruct((3, rows, width), BF16)] * pieces,
        in_specs=[smem(), anywhere(), anywhere(), anywhere()],
        out_specs=[vmem()] * pieces,
        scratch_shapes=[pltpu.SemaphoreType.DMA((pieces, 3))],
        name="pack",
    )(columns, queries, keys, values)


def attend_body(rows_at, *refs, pieces, slots, group, scale):
    parts = refs[:pieces]
    outs = refs[pieces : pieces + slots]
    mixed_ref, staged_ref = refs[pieces + slots :]
    rows = parts[0].shape[1]
    width = parts[0].shape[2]
    kept = rows // POOL
    block = outs[0].shape[0]
    ones = jnp.ones((pieces * rows, HD), BF16)
    for h in range(width // HD):
        cols = slice(h * HD, (h + 1) * HD)
        keys = jnp.concatenate([r[1, :, cols] for r in parts], axis=0)
        values = jnp.concatenate(
            [jnp.concatenate([r[2, :, cols] for r in parts], axis=0), ones], axis=1
        )
        for g in range(0, pieces, group):
            members = range(g, min(g + group, pieces))
            query = jnp.concatenate([parts[p][0, :, cols] for p in members], axis=0)
            scores = lax.dot_general(
                query, keys, (((1,), (1,)), ((), ())), preferred_element_type=F32
            )
            peak = jnp.max(scores, axis=1, keepdims=True)
            weights = jnp.exp2((scores - peak) * scale).astype(BF16)
            mixed = jnp.dot(weights, values, preferred_element_type=F32)
            mixed_ref[: len(members) * rows, :] = mixed[:, :HD] / mixed[:, HD:]
            for n, p in enumerate(members):
                total = sum(
                    mixed_ref[pl.ds(n * rows + r, kept, stride=POOL), :] for r in range(POOL)
                )
                start = pl.multiple_of(rows_at[p], kept)
                staged_ref[pl.ds(start, kept), cols] = (total / POOL).astype(BF16)
    for s in range(slots):
        outs[s][...] = staged_ref[s * block : (s + 1) * block, :]


def attend(rows_at, parts, slots, block):
    pieces = len(parts)
    rows, width = parts[0].shape[1:]
    group = max(1, min(pieces, 256 // rows))
    work = pieces * rows * pieces * rows * width * 2
    return pl.pallas_call(
        functools.partial(
            attend_body,
            pieces=pieces,
            slots=slots,
            group=group,
            scale=HD ** (-0.5) * math.log2(math.e),
        ),
        out_shape=[jax.ShapeDtypeStruct((block, width), BF16)] * slots,
        in_specs=[smem()] + [vmem()] * pieces,
        out_specs=[vmem()] * slots,
        scratch_shapes=[
            pltpu.VMEM((group * rows, HD), F32),
            pltpu.VMEM((slots * block, width), BF16),
        ],
        cost_estimate=pl.CostEstimate(
            flops=2 * work, bytes_accessed=0, transcendentals=work // (2 * HD)
        ),
        name="attend",
    )(rows_at, *parts)


def join_body(*refs):
    out = refs[-1]
    block = refs[0].shape[0]
    for s, r in enumerate(refs[:-1]):
        out[s * block : (s + 1) * block, :] = r[...]


def join(blocks):
    block, width = blocks[0].shape
    return pl.pallas_call(
        join_body,
        out_shape=jax.ShapeDtypeStruct((block * len(blocks), width), BF16),
        in_specs=[vmem()] * len(blocks),
        out_specs=vmem(),
        name="join",
    )(*blocks)


def product(at, parts, w_ref, first):
    total = None
    width = parts[0].shape[1]
    for p, part in enumerate(parts):
        start = pl.multiple_of(at[p] + first, HD)
        term = jnp.dot(part[...], w_ref[pl.ds(start, width), :], preferred_element_type=F32)
        total = term if total is None else total + term
    return total


def project_body(at, *refs, pieces, first):
    parts, w_ref, out = refs[:pieces], refs[pieces], refs[-1]
    out[...] = product(at, parts, w_ref, first)


def project(at, parts, w_proj, first):
    rows, width = parts[0].shape
    return pl.pallas_call(
        functools.partial(project_body, pieces=len(parts), first=first),
        out_shape=jax.ShapeDtypeStruct((rows, w_proj.shape[1]), F32),
        in_specs=[smem()] + [vmem()] * (len(parts) + 1),
        out_specs=vmem(),
        cost_estimate=pl.CostEstimate(
            flops=2 * rows * width * len(parts) * w_proj.shape[1],
            bytes_accessed=0,
            transcendentals=0,
        ),
        name="project",
    )(at, *parts, w_proj)


def hide_body(at, slot_of, limit_of, *refs, pieces, first, slots, carried):
    parts, w_ref, text_ref = refs[:pieces], refs[pieces], refs[pieces + 1]
    hidden_ref, square_ref = refs[-2:]
    total = product(at, parts, w_ref, first)
    if carried:
        total = total + refs[pieces + 2][...]
    rows, width = hidden_ref.shape
    block = rows // slots
    row_ids = lax.broadcasted_iota(jnp.int32, (block, width), 0)
    for s in range(slots):
        start = pl.multiple_of(slot_of[s] * block, block)
        live = row_ids < limit_of[s]
        hidden_ref[pl.ds(start, block), :] = jnp.where(
            live,
            total[s * block : (s + 1) * block, :],
            text_ref[pl.ds(start, block), :].astype(F32),
        )
    partial = None
    for c in range(0, width, 128):
        value = hidden_ref[:, c : c + 128]
        partial = value * value if partial is None else partial + value * value
    square_ref[...] = jnp.sum(partial.T, axis=0, keepdims=True)


def hide(at, slot_of, limit_of, parts, w_proj, text, carry, first, slots):
    rows, width = text.shape
    carried = carry is not None
    return pl.pallas_call(
        functools.partial(
            hide_body, pieces=len(parts), first=first, slots=slots, carried=carried
        ),
        out_shape=[
            jax.ShapeDtypeStruct((rows, width), F32),
            jax.ShapeDtypeStruct((1, rows), F32),
        ],
        in_specs=[smem()] * 3 + [vmem()] * (len(parts) + 2 + carried),
        out_specs=[vmem()] * 2,
        name="hide",
    )(at, slot_of, limit_of, *parts, w_proj, text, *([carry] if carried else []))


def norm_body(*refs, features):
    hidden_ref, gain_ref, out = refs[0], refs[1], refs[-1]
    total = sum(r[...] for r in refs[2:-1])
    inverse = lax.rsqrt(total / features + EPSILON)
    rows, width = hidden_ref.shape
    column = jnp.broadcast_to(inverse, (128, rows)).T
    for c in range(0, width, 128):
        out[:, c : c + 128] = (
            hidden_ref[:, c : c + 128] * column * gain_ref[:, c : c + 128]
        ).astype(BF16)


def norm(hidden, gain, sums, features):
    return pl.pallas_call(
        functools.partial(norm_body, features=features),
        out_shape=jax.ShapeDtypeStruct(hidden.shape, BF16),
        in_specs=[vmem()] * (2 + len(sums)),
        out_specs=vmem(),
        name="norm",
    )(hidden, gain, *sums)


def on_device(queries, keys, values, counts, offsets, text, w_proj, gain):
    members = lax.axis_size("seq")
    owners = lax.axis_size("img")
    me = lax.axis_index("seq")
    owner = lax.axis_index("img")
    rows = queries.shape[1]
    own_width = queries.shape[2] // members
    heads = own_width // HD
    kept = rows // POOL
    pool_count = kept * members
    block = pool_count // owners
    chips = members // 2

    def swap(x, axis, size, k):
        return lax.ppermute(x, axis, [(j, j ^ k) for j in range(size)])

    seq_ids = jnp.arange(members, dtype=jnp.int32) ^ me
    img_ids = jnp.arange(owners, dtype=jnp.int32)
    columns = seq_ids * own_width

    own_owner = lax.dynamic_slice_in_dim(offsets, owner, 1, 0)[0] // pool_count
    token = seq_ids * kept
    hit = (token // block)[:, None] == img_ids[None, :]
    target = jnp.sum(jnp.where(hit, own_owner[None, :], 0), axis=1)
    rows_at = (target ^ owner) * block + token % block

    landing = offsets // pool_count == owner
    slot_of_image = jnp.sum(jnp.where(landing, offsets % pool_count // block, 0), axis=1)
    block_of_image = jnp.sum(jnp.where(landing, img_ids[None, :], 0), axis=1)
    limit_of_image = counts - block_of_image * block
    source = (img_ids ^ owner)[:, None] == img_ids[None, :]
    slot_of = jnp.sum(jnp.where(source, slot_of_image[None, :], 0), axis=1)
    limit_of = jnp.sum(jnp.where(source, limit_of_image[None, :], 0), axis=1)

    spans = []
    first = 0
    for count in chunk_heads(heads):
        spans.append((first * HD, count * HD))
        first += count

    seq_order = sorted(range(1, members), key=lambda k: (-(k // 2).bit_count(), k))
    received = []
    for first, width in spans:
        sent = pack(columns, queries, keys, values, members, first, width)
        parts = [sent[0]] + [None] * (members - 1)
        for k in seq_order:
            parts[k] = swap(sent[k], "seq", members, k)
        received.append(parts)

    img_order = sorted(range(1, owners), key=lambda k: -k)
    chip_order = sorted(range(1, chips), key=lambda k: (-k.bit_count(), k))
    feature_order = [(members, 2 * c) for c in range(chips)] + [
        (members, 2 * c + 1) for c in range(chips)
    ]
    at = jnp.stack([seq_ids[k] * own_width for _, k in feature_order])
    gathered = []
    for parts, (first, width) in zip(received, spans):
        outgoing = attend(rows_at, parts, owners, block)
        blocks = [outgoing[0]] + [None] * (owners - 1)
        for k in img_order:
            blocks[k] = swap(outgoing[k], "img", owners, k)
        visual = join(blocks)
        near = [visual] + [None] * (chips - 1)
        for k in chip_order:
            near[k] = swap(visual, "seq", members, 2 * k)
        far = [swap(x, "seq", members, 1) for x in near]
        gathered.append(near + far)

    carry = None
    for parts, (first, width) in zip(gathered[:-1], spans[:-1]):
        term = project(at, parts, w_proj, first)
        carry = term if carry is None else carry + term
    hidden, square = hide(
        at, slot_of, limit_of, gathered[-1], w_proj, text, carry, spans[-1][0], owners
    )
    near = [square] + [swap(square, "seq", members, 2 * k) for k in chip_order]
    sums = near + [swap(x, "seq", members, 1) for x in near]
    return norm(hidden, gain[None, :], sums, members * text.shape[1])


def solution(mesh):
    in_specs = (
        P("img", "seq", None),
        P("img", "seq", None),
        P("img", "seq", None),
        P(),
        P(),
        P("img", "seq"),
        P(None, "seq"),
        P("seq"),
    )
    out_specs = P("img", "seq")
    return jax.shard_map(
        on_device, mesh=mesh, in_specs=in_specs, out_specs=out_specs, check_vma=False
    )
```

```python
import functools
import math

import jax
import jax.numpy as jnp
from jax import lax
from jax.experimental import pallas as pl
from jax.experimental.pallas import tpu as pltpu
from jax.sharding import PartitionSpec as P

HD = 128
POOL = 4
EPSILON = 1e-05
BF16 = jnp.bfloat16
F32 = jnp.float32


def vmem():
    return pl.BlockSpec(memory_space=pltpu.VMEM)


def smem():
    return pl.BlockSpec(memory_space=pltpu.SMEM)


def hbm():
    return pl.BlockSpec(memory_space=pltpu.HBM)


def anywhere():
    return pl.BlockSpec(memory_space=pl.ANY)


def in_hbm(x):
    return pltpu.with_memory_space_constraint(x, pltpu.HBM)


def hold_body(src, after, out, sem):
    copy = pltpu.make_async_copy(src, out, sem)
    copy.start()
    copy.wait()


def hold(array, after):
    return pl.pallas_call(
        hold_body,
        out_shape=jax.ShapeDtypeStruct(array.shape, array.dtype),
        in_specs=[hbm(), anywhere()],
        out_specs=vmem(),
        scratch_shapes=[pltpu.SemaphoreType.DMA],
        compiler_params=limit(10),
        name="hold",
    )(in_hbm(array), after)


def limit(mib):
    return pltpu.CompilerParams(vmem_limit_bytes=mib * 2**20)


def chunk_heads(heads):
    return [heads]


def pack_body(*refs, pieces, first, width):
    me = lax.axis_index("seq")
    q_ref, k_ref, v_ref = refs[:3]
    outs, sems = refs[-1 - pieces : -1], refs[-1]
    copies = []
    own_width = q_ref.shape[2] // pieces
    for p in range(pieces):
        start = pl.multiple_of((me ^ p) * own_width + first, HD)
        for t, src in enumerate((q_ref, k_ref, v_ref)):
            copies.append(
                pltpu.make_async_copy(
                    src.at[0, :, pl.ds(start, width)], outs[p].at[t], sems.at[p, t]
                )
            )
    for c in copies:
        c.start()
    for c in copies:
        c.wait()


def pack(queries, keys, values, pieces, first, width, after):
    rows = queries.shape[1]
    return pl.pallas_call(
        functools.partial(pack_body, pieces=pieces, first=first, width=width),
        out_shape=[jax.ShapeDtypeStruct((3, rows, width), BF16)] * pieces,
        in_specs=[hbm()] * 3 + [anywhere()] * len(after),
        out_specs=[vmem()] * pieces,
        scratch_shapes=[pltpu.SemaphoreType.DMA((pieces, 3))],
        compiler_params=limit(4),
        name="pack",
    )(in_hbm(queries), in_hbm(keys), in_hbm(values), *after)


def attend_body(rows_at, after, *refs, pieces, slots, group, scale):
    parts = refs[:pieces]
    outs = refs[pieces : pieces + slots]
    mixed_ref, staged_ref = refs[pieces + slots :]
    rows = parts[0].shape[1]
    width = parts[0].shape[2]
    kept = rows // POOL
    block = outs[0].shape[0]
    ones = jnp.ones((pieces * rows, HD), BF16)
    for h in range(width // HD):
        cols = slice(h * HD, (h + 1) * HD)
        keys = jnp.concatenate([r[1, :, cols] for r in parts], axis=0)
        values = jnp.concatenate(
            [jnp.concatenate([r[2, :, cols] for r in parts], axis=0), ones], axis=1
        )
        for g in range(0, pieces, group):
            members = range(g, min(g + group, pieces))
            query = jnp.concatenate([parts[p][0, :, cols] for p in members], axis=0)
            scores = lax.dot_general(
                query, keys, (((1,), (1,)), ((), ())), preferred_element_type=F32
            )
            peak = jnp.max(scores, axis=1, keepdims=True)
            weights = jnp.exp2((scores - peak) * scale).astype(BF16)
            mixed = jnp.dot(weights, values, preferred_element_type=F32)
            mixed_ref[: len(members) * rows, :] = mixed[:, :HD] / mixed[:, HD:]
            for n, p in enumerate(members):
                total = sum(
                    mixed_ref[pl.ds(n * rows + r, kept, stride=POOL), :] for r in range(POOL)
                )
                start = pl.multiple_of(rows_at[p], kept)
                staged_ref[pl.ds(start, kept), cols] = (total / POOL).astype(BF16)
    for s in range(slots):
        outs[s][...] = staged_ref[s * block : (s + 1) * block, :]


def attend(rows_at, after, parts, slots, block):
    pieces = len(parts)
    rows, width = parts[0].shape[1:]
    group = max(1, min(pieces, 256 // rows))
    work = pieces * rows * pieces * rows * width * 2
    return pl.pallas_call(
        functools.partial(
            attend_body,
            pieces=pieces,
            slots=slots,
            group=group,
            scale=HD ** (-0.5) * math.log2(math.e),
        ),
        out_shape=[jax.ShapeDtypeStruct((block, width), BF16)] * slots,
        in_specs=[smem(), anywhere()] + [vmem()] * pieces,
        out_specs=[vmem()] * slots,
        scratch_shapes=[
            pltpu.VMEM((group * rows, HD), F32),
            pltpu.VMEM((slots * block, width), BF16),
        ],
        cost_estimate=pl.CostEstimate(
            flops=2 * work, bytes_accessed=0, transcendentals=work // (2 * HD)
        ),
        compiler_params=limit(12),
        name="attend",
    )(rows_at, after, *parts)


def join_body(*refs):
    out = refs[-1]
    block = refs[0].shape[0]
    for s, r in enumerate(refs[:-1]):
        out[s * block : (s + 1) * block, :] = r[...]


def join(blocks):
    block, width = blocks[0].shape
    return pl.pallas_call(
        join_body,
        out_shape=jax.ShapeDtypeStruct((block * len(blocks), width), BF16),
        in_specs=[vmem()] * len(blocks),
        out_specs=vmem(),
        compiler_params=limit(2),
        name="join",
    )(*blocks)


def product(at, parts, w_ref, first):
    total = None
    width = parts[0].shape[1]
    for p, part in enumerate(parts):
        start = pl.multiple_of(at[p] + first, HD)
        term = jnp.dot(part[...], w_ref[pl.ds(start, width), :], preferred_element_type=F32)
        total = term if total is None else total + term
    return total


def project_body(at, *refs, pieces, first):
    parts, w_ref, out = refs[:pieces], refs[pieces], refs[-1]
    out[...] = product(at, parts, w_ref, first)


def project(at, parts, w_proj, first):
    rows, width = parts[0].shape
    return pl.pallas_call(
        functools.partial(project_body, pieces=len(parts), first=first),
        out_shape=jax.ShapeDtypeStruct((rows, w_proj.shape[1]), F32),
        in_specs=[smem()] + [vmem()] * (len(parts) + 1),
        out_specs=vmem(),
        cost_estimate=pl.CostEstimate(
            flops=2 * rows * width * len(parts) * w_proj.shape[1],
            bytes_accessed=0,
            transcendentals=0,
        ),
        compiler_params=limit(14),
        name="project",
    )(at, *parts, w_proj)


def hide_body(at, slot_of, limit_of, *refs, pieces, first, slots, carried):
    parts, w_ref, text_ref = refs[:pieces], refs[pieces], refs[pieces + 1]
    hidden_ref, square_ref = refs[-2:]
    total = product(at, parts, w_ref, first)
    if carried:
        total = total + refs[pieces + 2][...]
    rows, width = hidden_ref.shape
    block = rows // slots
    row_ids = lax.broadcasted_iota(jnp.int32, (block, width), 0)
    for s in range(slots):
        start = pl.multiple_of(slot_of[s] * block, block)
        live = row_ids < limit_of[s]
        hidden_ref[pl.ds(start, block), :] = jnp.where(
            live,
            total[s * block : (s + 1) * block, :],
            text_ref[pl.ds(start, block), :].astype(F32),
        )
    partial = None
    for c in range(0, width, 128):
        value = hidden_ref[:, c : c + 128]
        partial = value * value if partial is None else partial + value * value
    square_ref[...] = jnp.sum(partial.T, axis=0, keepdims=True)


def hide(at, slot_of, limit_of, parts, w_proj, text, carry, first, slots):
    rows, width = text.shape
    carried = carry is not None
    return pl.pallas_call(
        functools.partial(
            hide_body, pieces=len(parts), first=first, slots=slots, carried=carried
        ),
        out_shape=[
            jax.ShapeDtypeStruct((rows, width), F32),
            jax.ShapeDtypeStruct((1, rows), F32),
        ],
        in_specs=[smem()] * 3 + [vmem()] * (len(parts) + 2 + carried),
        out_specs=[vmem()] * 2,
        compiler_params=limit(18),
        name="hide",
    )(at, slot_of, limit_of, *parts, w_proj, text, *([carry] if carried else []))


def norm_body(*refs, features):
    hidden_ref, gain_ref, out = refs[0], refs[1], refs[-1]
    total = sum(r[...] for r in refs[2:-1])
    inverse = lax.rsqrt(total / features + EPSILON)
    rows, width = hidden_ref.shape
    column = jnp.broadcast_to(inverse, (128, rows)).T
    for c in range(0, width, 128):
        out[:, c : c + 128] = (
            hidden_ref[:, c : c + 128] * column * gain_ref[:, c : c + 128]
        ).astype(BF16)


def norm(hidden, gain, sums, features):
    return pl.pallas_call(
        functools.partial(norm_body, features=features),
        out_shape=jax.ShapeDtypeStruct(hidden.shape, BF16),
        in_specs=[vmem()] * (2 + len(sums)),
        out_specs=vmem(),
        compiler_params=limit(4),
        name="norm",
    )(hidden, gain, *sums)


def on_device(queries, keys, values, counts, offsets, text, w_proj, gain):
    members = lax.axis_size("seq")
    owners = lax.axis_size("img")
    me = lax.axis_index("seq")
    owner = lax.axis_index("img")
    rows = queries.shape[1]
    own_width = queries.shape[2] // members
    heads = own_width // HD
    kept = rows // POOL
    pool_count = kept * members
    block = pool_count // owners
    chips = members // 2

    def swap(x, axis, size, k):
        return lax.ppermute(x, axis, [(j, j ^ k) for j in range(size)])

    seq_ids = jnp.arange(members, dtype=jnp.int32) ^ me
    img_ids = jnp.arange(owners, dtype=jnp.int32)

    own_owner = lax.dynamic_slice_in_dim(offsets, owner, 1, 0)[0] // pool_count
    token = seq_ids * kept
    hit = (token // block)[:, None] == img_ids[None, :]
    target = jnp.sum(jnp.where(hit, own_owner[None, :], 0), axis=1)
    rows_at = (target ^ owner) * block + token % block

    landing = offsets // pool_count == owner
    slot_of_image = jnp.sum(jnp.where(landing, offsets % pool_count // block, 0), axis=1)
    block_of_image = jnp.sum(jnp.where(landing, img_ids[None, :], 0), axis=1)
    limit_of_image = counts - block_of_image * block
    source = (img_ids ^ owner)[:, None] == img_ids[None, :]
    slot_of = jnp.sum(jnp.where(source, slot_of_image[None, :], 0), axis=1)
    limit_of = jnp.sum(jnp.where(source, limit_of_image[None, :], 0), axis=1)

    spans = []
    first = 0
    for count in chunk_heads(heads):
        spans.append((first * HD, count * HD))
        first += count

    seq_order = sorted(range(1, members), key=lambda k: (-(k // 2).bit_count(), k))
    received = []
    for first, width in spans:
        after = [received[-1][0]] if received else []
        sent = pack(queries, keys, values, members, first, width, after)
        parts = [sent[0]] + [None] * (members - 1)
        for k in seq_order:
            parts[k] = swap(sent[k], "seq", members, k)
        received.append(parts)
    weight = hold(w_proj, received[-1][0])

    img_order = sorted(range(1, owners), key=lambda k: -k)
    chip_order = sorted(range(1, chips), key=lambda k: (-k.bit_count(), k))
    senders = jnp.arange(chips, dtype=jnp.int32) * 2
    at = (jnp.concatenate([senders, senders + 1]) ^ me) * own_width
    gathered = []
    for parts, (first, width) in zip(received, spans):
        outgoing = attend(rows_at, weight, parts, owners, block)
        blocks = [outgoing[0]] + [None] * (owners - 1)
        for k in img_order:
            blocks[k] = swap(outgoing[k], "img", owners, k)
        visual = join(blocks)
        near = [visual] + [None] * (chips - 1)
        for k in chip_order:
            near[k] = swap(visual, "seq", members, 2 * k)
        far = [swap(x, "seq", members, 1) for x in near]
        gathered.append(near + far)

    carry = None
    for parts, (first, width) in zip(gathered[:-1], spans[:-1]):
        term = project(at, parts, weight, first)
        carry = term if carry is None else carry + term
    hidden, square = hide(
        at, slot_of, limit_of, gathered[-1], weight, text, carry, spans[-1][0], owners
    )
    near = [square] + [swap(square, "seq", members, 2 * k) for k in chip_order]
    sums = near + [swap(x, "seq", members, 1) for x in near]
    return norm(hidden, gain[None, :], sums, members * text.shape[1])


def solution(mesh):
    in_specs = (
        P("img", "seq", None),
        P("img", "seq", None),
        P("img", "seq", None),
        P(),
        P(),
        P("img", "seq"),
        P(None, "seq"),
        P("seq"),
    )
    out_specs = P("img", "seq")
    return jax.shard_map(
        on_device, mesh=mesh, in_specs=in_specs, out_specs=out_specs, check_vma=False
    )
```

```python
import functools
import math

import jax
import jax.numpy as jnp
from jax import lax
from jax.experimental import pallas as pl
from jax.experimental.pallas import tpu as pltpu
from jax.sharding import PartitionSpec as P


HD = 128
POOL = 4
EPSILON = 1e-05
BF16 = jnp.bfloat16
F32 = jnp.float32


def vmem():
    return pl.BlockSpec(memory_space=pltpu.VMEM)


def smem():
    return pl.BlockSpec(memory_space=pltpu.SMEM)


def hbm():
    return pl.BlockSpec(memory_space=pltpu.HBM)


def anywhere():
    return pl.BlockSpec(memory_space=pl.ANY)


def in_hbm(x):
    return pltpu.with_memory_space_constraint(x, pltpu.HBM)


def hold_body(src, after, out, sem):
    copy = pltpu.make_async_copy(src, out, sem)
    copy.start()
    copy.wait()


def hold(array, after):
    return pl.pallas_call(
        hold_body,
        out_shape=jax.ShapeDtypeStruct(array.shape, array.dtype),
        in_specs=[hbm(), anywhere()],
        out_specs=vmem(),
        scratch_shapes=[pltpu.SemaphoreType.DMA],
        compiler_params=limit(10),
        name="hold",
    )(in_hbm(array), after)


def limit(mib):
    return pltpu.CompilerParams(vmem_limit_bytes=mib * 2**20)


def pack_body(*refs, pieces, tensors):
    me = lax.axis_index("seq")
    sources = refs[:tensors]
    outs, sems = refs[-1 - pieces : -1], refs[-1]
    width = outs[0].shape[2]
    copies = []
    for p in range(pieces):
        start = pl.multiple_of((me ^ p) * width, HD)
        for t, src in enumerate(sources):
            copies.append(
                pltpu.make_async_copy(
                    src.at[0, :, pl.ds(start, width)], outs[p].at[t], sems.at[p, t]
                )
            )
    for c in copies:
        c.start()
    for c in copies:
        c.wait()


def pack(tensors, pieces):
    rows = tensors[0].shape[1]
    width = tensors[0].shape[2] // pieces
    count = len(tensors)
    return pl.pallas_call(
        functools.partial(pack_body, pieces=pieces, tensors=count),
        out_shape=[jax.ShapeDtypeStruct((count, rows, width), BF16)] * pieces,
        in_specs=[hbm()] * count,
        out_specs=[vmem()] * pieces,
        scratch_shapes=[pltpu.SemaphoreType.DMA((pieces, count))],
        compiler_params=limit(4),
        name="pack",
    )(*[in_hbm(t) for t in tensors])


def score_body(after, *refs, scale):
    parts, out = refs[:-1], refs[-1]
    pieces = len(parts)
    rows, width = parts[0].shape[1:]
    group = max(1, min(pieces, 256 // rows))
    for h in range(width // HD):
        cols = slice(h * HD, (h + 1) * HD)
        keys = jnp.concatenate([r[1, :, cols] for r in parts], axis=0)
        for g in range(0, pieces, group):
            query = jnp.concatenate([r[0, :, cols] for r in parts[g : g + group]], axis=0)
            scores = lax.dot_general(
                query, keys, (((1,), (1,)), ((), ())), preferred_element_type=F32
            )
            peak = jnp.max(scores, axis=1, keepdims=True)
            out[h, g * rows : g * rows + query.shape[0], :] = jnp.exp2(
                (scores - peak) * scale
            ).astype(BF16)


def score(after, parts):
    rows, width = parts[0].shape[1:]
    keys = len(parts) * rows
    heads = width // HD
    return pl.pallas_call(
        functools.partial(score_body, scale=HD ** (-0.5) * math.log2(math.e)),
        out_shape=jax.ShapeDtypeStruct((heads, keys, keys), BF16),
        in_specs=[anywhere()] + [vmem()] * len(parts),
        out_specs=vmem(),
        compiler_params=limit(14),
        cost_estimate=pl.CostEstimate(
            flops=2 * keys * keys * width,
            bytes_accessed=0,
            transcendentals=keys * keys * heads,
        ),
        name="score",
    )(after, *parts)


def mix_body(rows_at, weight_ref, *refs, ids, slots):
    pieces = len(ids)
    parts = refs[:pieces]
    outs = refs[pieces : pieces + slots]
    mixed_ref, staged_ref = refs[pieces + slots :]
    rows = parts[0].shape[1]
    kept = rows // POOL
    block = outs[0].shape[0]
    ones = jnp.ones((pieces * rows, HD), BF16)
    for h in range(weight_ref.shape[0]):
        cols = slice(h * HD, (h + 1) * HD)
        values = jnp.concatenate(
            [jnp.concatenate([r[0, :, cols] for r in parts], axis=0), ones], axis=1
        )
        mixed = jnp.dot(weight_ref[h], values, preferred_element_type=F32)
        mixed_ref[...] = mixed[:, :HD] / mixed[:, HD:]
        for p in range(pieces):
            total = sum(
                mixed_ref[pl.ds(p * rows + r, kept, stride=POOL), :] for r in range(POOL)
            )
            start = pl.multiple_of(rows_at[ids[p]], kept)
            staged_ref[pl.ds(start, kept), cols] = (total / POOL).astype(BF16)
    for s in range(slots):
        outs[s][...] = staged_ref[s * block : (s + 1) * block, :]


def mix(rows_at, weights, ids, parts, slots, block):
    rows, width = parts[0].shape[1:]
    return pl.pallas_call(
        functools.partial(mix_body, ids=ids, slots=slots),
        out_shape=[jax.ShapeDtypeStruct((block, width), BF16)] * slots,
        in_specs=[smem(), vmem()] + [vmem()] * len(parts),
        out_specs=[vmem()] * slots,
        scratch_shapes=[
            pltpu.VMEM((len(parts) * rows, HD), F32),
            pltpu.VMEM((slots * block, width), BF16),
        ],
        compiler_params=limit(20),
        name="mix",
    )(rows_at, weights, *parts)


def join_body(*refs):
    out = refs[-1]
    block = refs[0].shape[0]
    for s, r in enumerate(refs[:-1]):
        out[s * block : (s + 1) * block, :] = r[...]


def join(blocks):
    block, width = blocks[0].shape
    return pl.pallas_call(
        join_body,
        out_shape=jax.ShapeDtypeStruct((block * len(blocks), width), BF16),
        in_specs=[vmem()] * len(blocks),
        out_specs=vmem(),
        compiler_params=limit(2),
        name="join",
    )(*blocks)


def product(at, ids, parts, w_ref):
    total = None
    width = parts[0].shape[1]
    for n, part in zip(ids, parts):
        start = pl.multiple_of(at[n], HD)
        term = jnp.dot(part[...], w_ref[pl.ds(start, width), :], preferred_element_type=F32)
        total = term if total is None else total + term
    return total


def project_body(at, *refs, ids, carried):
    pieces = len(ids)
    parts, w_ref, out = refs[:pieces], refs[pieces], refs[-1]
    total = product(at, ids, parts, w_ref)
    if carried:
        total = total + refs[pieces + 1][...]
    out[...] = total


def project(at, ids, parts, w_proj, carry):
    rows, width = parts[0].shape
    carried = carry is not None
    return pl.pallas_call(
        functools.partial(project_body, ids=ids, carried=carried),
        out_shape=jax.ShapeDtypeStruct((rows, w_proj.shape[1]), F32),
        in_specs=[smem()] + [vmem()] * (len(parts) + 1 + carried),
        out_specs=vmem(),
        cost_estimate=pl.CostEstimate(
            flops=2 * rows * width * len(parts) * w_proj.shape[1],
            bytes_accessed=0,
            transcendentals=0,
        ),
        compiler_params=limit(14),
        name="project",
    )(at, *parts, w_proj, *([carry] if carried else []))


def hide_body(at, slot_of, limit_of, *refs, ids, slots, carried):
    pieces = len(ids)
    parts, w_ref, text_ref = refs[:pieces], refs[pieces], refs[pieces + 1]
    hidden_ref, square_ref = refs[-2:]
    total = product(at, ids, parts, w_ref)
    if carried:
        total = total + refs[pieces + 2][...]
    rows, width = hidden_ref.shape
    block = rows // slots
    row_ids = lax.broadcasted_iota(jnp.int32, (block, width), 0)
    for s in range(slots):
        start = pl.multiple_of(slot_of[s] * block, block)
        live = row_ids < limit_of[s]
        hidden_ref[pl.ds(start, block), :] = jnp.where(
            live,
            total[s * block : (s + 1) * block, :],
            text_ref[pl.ds(start, block), :].astype(F32),
        )
    partial = None
    for c in range(0, width, 128):
        value = hidden_ref[:, c : c + 128]
        partial = value * value if partial is None else partial + value * value
    square_ref[...] = jnp.sum(partial.T, axis=0, keepdims=True)


def hide(at, slot_of, limit_of, ids, parts, w_proj, text, carry, slots):
    rows, width = text.shape
    carried = carry is not None
    return pl.pallas_call(
        functools.partial(
            hide_body, ids=ids, slots=slots, carried=carried
        ),
        out_shape=[
            jax.ShapeDtypeStruct((rows, width), F32),
            jax.ShapeDtypeStruct((1, rows), F32),
        ],
        in_specs=[smem()] * 3 + [vmem()] * (len(parts) + 2 + carried),
        out_specs=[vmem()] * 2,
        compiler_params=limit(18),
        name="hide",
    )(at, slot_of, limit_of, *parts, w_proj, text, *([carry] if carried else []))


def norm_body(*refs, features):
    hidden_ref, gain_ref, out = refs[0], refs[1], refs[-1]
    total = sum(r[...] for r in refs[2:-1])
    inverse = lax.rsqrt(total / features + EPSILON)
    rows, width = hidden_ref.shape
    column = jnp.broadcast_to(inverse, (128, rows)).T
    for c in range(0, width, 128):
        out[:, c : c + 128] = (
            hidden_ref[:, c : c + 128] * column * gain_ref[:, c : c + 128]
        ).astype(BF16)


def norm(hidden, gain, sums, features):
    return pl.pallas_call(
        functools.partial(norm_body, features=features),
        out_shape=jax.ShapeDtypeStruct(hidden.shape, BF16),
        in_specs=[vmem()] * (2 + len(sums)),
        out_specs=vmem(),
        compiler_params=limit(4),
        name="norm",
    )(hidden, gain, *sums)


def on_device(queries, keys, values, counts, offsets, text, w_proj, gain):
    members = lax.axis_size("seq")
    owners = lax.axis_size("img")
    me = lax.axis_index("seq")
    owner = lax.axis_index("img")
    rows = queries.shape[1]
    own_width = queries.shape[2] // members
    kept = rows // POOL
    pool_count = kept * members
    block = pool_count // owners
    chips = members // 2

    def swap(x, axis, k):
        pairs = [(j, j ^ k) for j in range(lax.axis_size(axis))]
        return lax.ppermute(x, axis, pairs)

    seq_ids = jnp.arange(members, dtype=jnp.int32) ^ me
    img_ids = jnp.arange(owners, dtype=jnp.int32)

    own_owner = lax.dynamic_slice_in_dim(offsets, owner, 1, 0)[0] // pool_count
    token = seq_ids * kept
    hit = (token // block)[:, None] == img_ids[None, :]
    target = jnp.sum(jnp.where(hit, own_owner[None, :], 0), axis=1)
    rows_at = (target ^ owner) * block + token % block

    landing = offsets // pool_count == owner
    slot_of_image = jnp.sum(jnp.where(landing, offsets % pool_count // block, 0), axis=1)
    block_of_image = jnp.sum(jnp.where(landing, img_ids[None, :], 0), axis=1)
    limit_of_image = counts - block_of_image * block
    source = (img_ids ^ owner)[:, None] == img_ids[None, :]
    slot_of = jnp.sum(jnp.where(source, slot_of_image[None, :], 0), axis=1)
    limit_of = jnp.sum(jnp.where(source, limit_of_image[None, :], 0), axis=1)
    at = seq_ids * own_width

    order = seq_order(members)

    def exchange(tensors):
        sent = pack(tensors, members)
        return [sent[0]] + [swap(sent[k], "seq", k) for k in order[1:]]

    pairs = exchange([queries, keys])
    singles = exchange([values])
    weight = hold(w_proj, singles[0])
    weights = score(weight, pairs)
    outgoing = mix(rows_at, weights, order, singles, owners, block)
    blocks = [outgoing[0]] + [None] * (owners - 1)
    for k in img_order(owners):
        blocks[k] = swap(outgoing[k], "img", k)
    visual = join(blocks)
    near = {0: visual}
    for k in chip_order(chips):
        near[k] = swap(visual, "seq", 2 * k)
    far = {}
    for k, x in near.items():
        far[k] = swap(x, "seq", 1)
    carry = None
    levels = chips.bit_length()
    for hops in range(levels):
        level = [k for k in near if k.bit_count() == hops]
        ids = tuple(2 * k for k in level) + tuple(2 * k + 1 for k in level)
        parts = [near[k] for k in level] + [far[k] for k in level]
        if hops < levels - 1:
            carry = project(at, ids, parts, weight, carry)
    hidden, square = hide(at, slot_of, limit_of, ids, parts, weight, text, carry, owners)
    square = square + swap(square, "seq", 1)
    sums = [square] + [swap(square, "seq", 2 * k) for k in chip_order(chips)]
    return norm(hidden, gain[None, :], sums, members * text.shape[1])


def seq_order(members):
    cross = sorted(range(2, members), key=lambda k: ((k // 2).bit_count(), k % 2, k))
    return (0, *cross, 1)


def img_order(owners):
    return sorted(range(1, owners), key=lambda k: -k)


def chip_order(chips):
    return sorted(range(1, chips), key=lambda k: (k.bit_count(), k))


def solution(mesh):
    in_specs = (
        P("img", "seq", None),
        P("img", "seq", None),
        P("img", "seq", None),
        P(),
        P(),
        P("img", "seq"),
        P(None, "seq"),
        P("seq"),
    )
    out_specs = P("img", "seq")
    return jax.shard_map(
        on_device, mesh=mesh, in_specs=in_specs, out_specs=out_specs, check_vma=False
    )
```

```python
import functools
import math

import jax
import jax.numpy as jnp
from jax import lax
from jax.experimental import pallas as pl
from jax.experimental.pallas import tpu as pltpu
from jax.sharding import PartitionSpec as P


HD = 128
POOL = 4
EPSILON = 1e-05
BF16 = jnp.bfloat16
F32 = jnp.float32


def vmem():
    return pl.BlockSpec(memory_space=pltpu.VMEM)


def smem():
    return pl.BlockSpec(memory_space=pltpu.SMEM)


def hbm():
    return pl.BlockSpec(memory_space=pltpu.HBM)


def anywhere():
    return pl.BlockSpec(memory_space=pl.ANY)


def in_hbm(x):
    return pltpu.with_memory_space_constraint(x, pltpu.HBM)


def hold_body(src, after, out, sem):
    copy = pltpu.make_async_copy(src, out, sem)
    copy.start()
    copy.wait()


def hold(array, after):
    return pl.pallas_call(
        hold_body,
        out_shape=jax.ShapeDtypeStruct(array.shape, array.dtype),
        in_specs=[hbm(), anywhere()],
        out_specs=vmem(),
        scratch_shapes=[pltpu.SemaphoreType.DMA],
        compiler_params=limit(10),
        name="hold",
    )(in_hbm(array), after)


def limit(mib):
    return pltpu.CompilerParams(vmem_limit_bytes=mib * 2**20)


def pack_body(*refs, pieces, tensors):
    me = lax.axis_index("seq")
    sources = refs[:tensors]
    outs, sems = refs[-1 - pieces : -1], refs[-1]
    width = outs[0].shape[2]
    copies = []
    for p in range(pieces):
        start = pl.multiple_of((me ^ p) * width, HD)
        for t, src in enumerate(sources):
            copies.append(
                pltpu.make_async_copy(
                    src.at[0, :, pl.ds(start, width)], outs[p].at[t], sems.at[p, t]
                )
            )
    for c in copies:
        c.start()
    for c in copies:
        c.wait()


def pack(tensors, pieces):
    rows = tensors[0].shape[1]
    width = tensors[0].shape[2] // pieces
    count = len(tensors)
    return pl.pallas_call(
        functools.partial(pack_body, pieces=pieces, tensors=count),
        out_shape=[jax.ShapeDtypeStruct((count, rows, width), BF16)] * pieces,
        in_specs=[hbm()] * count,
        out_specs=[vmem()] * pieces,
        scratch_shapes=[pltpu.SemaphoreType.DMA((pieces, count))],
        compiler_params=limit(4),
        name="pack",
    )(*[in_hbm(t) for t in tensors])


def score_body(after, *refs, scale):
    parts, out, staged_ref = refs[:-2], refs[-2], refs[-1]
    pieces = len(parts)
    rows, width = parts[0].shape[1:]
    group = max(1, min(pieces, 256 // rows))
    for h in range(width // HD):
        cols = slice(h * HD, (h + 1) * HD)
        keys = jnp.concatenate([r[1, :, cols] for r in parts], axis=0)
        for g in range(0, pieces, group):
            query = jnp.concatenate([r[0, :, cols] for r in parts[g : g + group]], axis=0)
            size = query.shape[0]
            scores = lax.dot_general(
                query, keys, (((1,), (1,)), ((), ())), preferred_element_type=F32
            )
            peak = jnp.max(scores, axis=1, keepdims=True)
            exponent = jnp.exp2((scores - peak) * scale)
            share = 1.0 / (POOL * jnp.sum(exponent, axis=1, keepdims=True))
            weights = exponent * share
            for c in range(pieces * rows // HD):
                staged_ref[c, :size, :] = weights[:, c * HD : (c + 1) * HD]
            for c in range(pieces * rows // HD):
                total = sum(
                    staged_ref[c, pl.ds(r, size // POOL, stride=POOL), :]
                    for r in range(POOL)
                )
                out[
                    h, g * rows // POOL : (g * rows + size) // POOL, c * HD : (c + 1) * HD
                ] = total.astype(BF16)


def score(after, parts):
    rows, width = parts[0].shape[1:]
    keys = len(parts) * rows
    heads = width // HD
    group = max(1, min(len(parts), 256 // rows))
    return pl.pallas_call(
        functools.partial(score_body, scale=HD ** (-0.5) * math.log2(math.e)),
        out_shape=jax.ShapeDtypeStruct((heads, keys // POOL, keys), BF16),
        in_specs=[anywhere()] + [vmem()] * len(parts),
        out_specs=vmem(),
        scratch_shapes=[pltpu.VMEM((keys // HD, group * rows, HD), F32)],
        compiler_params=limit(16),
        cost_estimate=pl.CostEstimate(
            flops=2 * keys * keys * width,
            bytes_accessed=0,
            transcendentals=keys * keys * heads,
        ),
        name="score",
    )(after, *parts)


def mix_body(offsets, weight_ref, *refs, ids, slots):
    pieces = len(ids)
    parts = refs[:pieces]
    outs = refs[pieces : pieces + slots]
    staged_ref = refs[pieces + slots]
    me, owner = lax.axis_index("seq"), lax.axis_index("img")
    kept = parts[0].shape[1] // POOL
    block = outs[0].shape[0]
    rows_at = []
    for k in ids:
        token = (me ^ k) * kept
        target = offsets[owner, token // block] // (kept * pieces)
        rows_at.append(pl.multiple_of((target ^ owner) * block + token % block, kept))
    for h in range(weight_ref.shape[0]):
        cols = slice(h * HD, (h + 1) * HD)
        values = jnp.concatenate([r[0, :, cols] for r in parts], axis=0)
        pooled = jnp.dot(weight_ref[h], values, preferred_element_type=F32).astype(BF16)
        for p, start in enumerate(rows_at):
            staged_ref[pl.ds(start, kept), cols] = pooled[p * kept : (p + 1) * kept, :]
    for s in range(slots):
        outs[s][...] = staged_ref[s * block : (s + 1) * block, :]


def mix(offsets, weights, ids, parts, slots, block):
    width = parts[0].shape[2]
    return pl.pallas_call(
        functools.partial(mix_body, ids=ids, slots=slots),
        out_shape=[jax.ShapeDtypeStruct((block, width), BF16)] * slots,
        in_specs=[smem(), vmem()] + [vmem()] * len(parts),
        out_specs=[vmem()] * slots,
        scratch_shapes=[pltpu.VMEM((slots * block, width), BF16)],
        compiler_params=limit(8),
        name="mix",
    )(offsets, weights, *parts)


def join_body(*refs):
    out = refs[-1]
    block = refs[0].shape[0]
    for s, r in enumerate(refs[:-1]):
        out[s * block : (s + 1) * block, :] = r[...]


def join(blocks):
    block, width = blocks[0].shape
    return pl.pallas_call(
        join_body,
        out_shape=jax.ShapeDtypeStruct((block * len(blocks), width), BF16),
        in_specs=[vmem()] * len(blocks),
        out_specs=vmem(),
        compiler_params=limit(2),
        name="join",
    )(*blocks)


def product(ids, parts, w_ref):
    me = lax.axis_index("seq")
    total = None
    width = parts[0].shape[1]
    for n, part in zip(ids, parts):
        start = pl.multiple_of((me ^ n) * width, HD)
        term = jnp.dot(part[...], w_ref[pl.ds(start, width), :], preferred_element_type=F32)
        total = term if total is None else total + term
    return total


def project_body(*refs, ids, carried):
    pieces = len(ids)
    parts, w_ref, out = refs[:pieces], refs[pieces], refs[-1]
    total = product(ids, parts, w_ref)
    if carried:
        total = total + refs[pieces + 1][...]
    out[...] = total


def project(ids, parts, w_proj, carry):
    rows, width = parts[0].shape
    carried = carry is not None
    return pl.pallas_call(
        functools.partial(project_body, ids=ids, carried=carried),
        out_shape=jax.ShapeDtypeStruct((rows, w_proj.shape[1]), F32),
        in_specs=[vmem()] * (len(parts) + 1 + carried),
        out_specs=vmem(),
        cost_estimate=pl.CostEstimate(
            flops=2 * rows * width * len(parts) * w_proj.shape[1],
            bytes_accessed=0,
            transcendentals=0,
        ),
        compiler_params=limit(14),
        name="project",
    )(*parts, w_proj, *([carry] if carried else []))


def hide_body(offsets, counts, *refs, ids, slots, carried):
    pieces = len(ids)
    parts, w_ref, text_ref = refs[:pieces], refs[pieces], refs[pieces + 1]
    hidden_ref, square_ref = refs[-2:]
    total = product(ids, parts, w_ref)
    if carried:
        total = total + refs[pieces + 2][...]
    rows, width = hidden_ref.shape
    block = rows // slots
    row_ids = lax.broadcasted_iota(jnp.int32, (block, width), 0)
    owner = lax.axis_index("img")
    for s in range(slots):
        source = owner ^ s

        def find(j, found):
            offset = offsets[source, j]
            here = offset // rows == owner
            return (
                jnp.where(here, offset - owner * rows, found[0]),
                jnp.where(here, counts[source] - j * block, found[1]),
            )

        found = lax.fori_loop(0, slots, find, (jnp.int32(0), jnp.int32(0)), unroll=slots <= 4)
        start = pl.multiple_of(found[0], block)
        live = row_ids < found[1]
        hidden_ref[pl.ds(start, block), :] = jnp.where(
            live,
            total[s * block : (s + 1) * block, :],
            text_ref[pl.ds(start, block), :].astype(F32),
        )
    partial = None
    for c in range(0, width, 128):
        value = hidden_ref[:, c : c + 128]
        partial = value * value if partial is None else partial + value * value
    square_ref[...] = jnp.sum(partial.T, axis=0, keepdims=True)


def hide(offsets, counts, ids, parts, w_proj, text, carry, slots):
    rows, width = text.shape
    carried = carry is not None
    return pl.pallas_call(
        functools.partial(
            hide_body, ids=ids, slots=slots, carried=carried
        ),
        out_shape=[
            jax.ShapeDtypeStruct((rows, width), F32),
            jax.ShapeDtypeStruct((1, rows), F32),
        ],
        in_specs=[smem()] * 2 + [vmem()] * (len(parts) + 2 + carried),
        out_specs=[vmem()] * 2,
        compiler_params=limit(18),
        name="hide",
    )(offsets, counts, *parts, w_proj, text, *([carry] if carried else []))


def norm_body(*refs, features):
    hidden_ref, gain_ref, out = refs[0], refs[1], refs[-1]
    total = sum(r[...] for r in refs[2:-1])
    inverse = lax.rsqrt(total / features + EPSILON)
    rows, width = hidden_ref.shape
    column = jnp.broadcast_to(inverse, (128, rows)).T
    for c in range(0, width, 128):
        out[:, c : c + 128] = (
            hidden_ref[:, c : c + 128] * column * gain_ref[:, c : c + 128]
        ).astype(BF16)


def norm(hidden, gain, sums, features):
    return pl.pallas_call(
        functools.partial(norm_body, features=features),
        out_shape=jax.ShapeDtypeStruct(hidden.shape, BF16),
        in_specs=[vmem()] * (2 + len(sums)),
        out_specs=vmem(),
        compiler_params=limit(4),
        name="norm",
    )(hidden, gain, *sums)


def on_device(queries, keys, values, counts, offsets, text, w_proj, gain):
    members = lax.axis_size("seq")
    owners = lax.axis_size("img")
    block = queries.shape[1] // POOL * members // owners
    chips = members // 2

    def swap(x, axis, k):
        pairs = [(j, j ^ k) for j in range(lax.axis_size(axis))]
        return lax.ppermute(x, axis, pairs)

    order = seq_order(members)

    def exchange(tensors):
        sent = pack(tensors, members)
        return [sent[0]] + [swap(sent[k], "seq", k) for k in order[1:]]

    pairs = exchange([queries, keys])
    singles = exchange([values])
    weight = hold(w_proj, singles[0])
    weights = score(weight, pairs)
    outgoing = mix(offsets, weights, order, singles, owners, block)
    blocks = [outgoing[0]] + [None] * (owners - 1)
    for k in img_order(owners):
        blocks[k] = swap(outgoing[k], "img", k)
    visual = join(blocks)
    near = {0: visual}
    for k in chip_order(chips):
        near[k] = swap(visual, "seq", 2 * k)
    far = {}
    for k, x in near.items():
        far[k] = swap(x, "seq", 1)
    carry = None
    steps = project_steps(chips)
    for n, ids in enumerate(steps):
        parts = [far[i // 2] if i % 2 else near[i // 2] for i in ids]
        if n < len(steps) - 1:
            carry = project(ids, parts, weight, carry)
    hidden, square = hide(offsets, counts, ids, parts, weight, text, carry, owners)
    square = square + swap(square, "seq", 1)
    sums = [square] + [swap(square, "seq", 2 * k + 1) for k in square_order(chips)]
    return norm(hidden, gain[None, :], sums, members * text.shape[1])


def seq_order(members):
    cross = sorted(range(2, members), key=lambda k: ((k // 2).bit_count(), k % 2, k))
    return (0, *cross, 1)


def img_order(owners):
    return sorted(range(1, owners), key=lambda k: (k == 1, k.bit_count(), k))


def chip_order(chips):
    return sorted(range(1, chips), key=lambda k: (k.bit_count(), k))


def square_order(chips):
    return sorted(range(1, chips), key=lambda k: -k)


def project_steps(chips):
    order = chip_order(chips)
    early = [i for k in order[:-2] for i in (2 * k, 2 * k + 1)]
    late = [i for k in order[-2:-1] for i in (2 * k, 2 * k + 1)]
    steps = [[0, 1], early, late + [2 * order[-1]], [2 * order[-1] + 1]]
    return [tuple(ids) for ids in steps if ids]


def solution(mesh):
    in_specs = (
        P("img", "seq", None),
        P("img", "seq", None),
        P("img", "seq", None),
        P(),
        P(),
        P("img", "seq"),
        P(None, "seq"),
        P("seq"),
    )
    out_specs = P("img", "seq")
    return jax.shard_map(
        on_device, mesh=mesh, in_specs=in_specs, out_specs=out_specs, check_vma=False
    )
```

```python
import functools
import math

import jax
import jax.numpy as jnp
from jax import lax
from jax.experimental import pallas as pl
from jax.experimental.pallas import tpu as pltpu
from jax.sharding import PartitionSpec as P


HD = 128
POOL = 4
EPSILON = 1e-05
BF16 = jnp.bfloat16
F32 = jnp.float32


def vmem():
    return pl.BlockSpec(memory_space=pltpu.VMEM)


def smem():
    return pl.BlockSpec(memory_space=pltpu.SMEM)


def hbm():
    return pl.BlockSpec(memory_space=pltpu.HBM)


def in_hbm(x):
    return pltpu.with_memory_space_constraint(x, pltpu.HBM)


def limit(mib):
    return pltpu.CompilerParams(vmem_limit_bytes=mib * 2**20)


def pack_body(*refs, pieces, tensors):
    me = lax.axis_index("seq")
    sources = refs[:tensors]
    outs, sems = refs[-1 - pieces : -1], refs[-1]
    width = outs[0].shape[2]
    copies = []
    for p in range(pieces):
        start = pl.multiple_of((me ^ p) * width, HD)
        for t, src in enumerate(sources):
            copies.append(
                pltpu.make_async_copy(
                    src.at[0, :, pl.ds(start, width)], outs[p].at[t], sems.at[p, t]
                )
            )
    for c in copies:
        c.start()
    for c in copies:
        c.wait()


def pack(tensors, pieces):
    rows = tensors[0].shape[1]
    width = tensors[0].shape[2] // pieces
    count = len(tensors)
    return pl.pallas_call(
        functools.partial(pack_body, pieces=pieces, tensors=count),
        out_shape=[jax.ShapeDtypeStruct((count, rows, width), BF16)] * pieces,
        in_specs=[hbm()] * count,
        out_specs=[vmem()] * pieces,
        scratch_shapes=[pltpu.SemaphoreType.DMA((pieces, count))],
        compiler_params=limit(4),
        name="pack",
    )(*[in_hbm(t) for t in tensors])


def score_body(offsets_ref, w_ref, *refs, ids, slots, scale):
    pieces = len(ids)
    parts = refs[:pieces]
    out, held_ref, staged_ref, offsets, sems = refs[pieces:]
    table = pltpu.make_async_copy(offsets_ref, offsets, sems.at[0])
    table.start()
    fetch = pltpu.make_async_copy(w_ref, held_ref, sems.at[1])
    fetch.start()
    rows, width = parts[0].shape[1:]
    kept = rows // POOL
    block = kept * pieces // slots
    me, owner = lax.axis_index("seq"), lax.axis_index("img")
    group = max(1, min(pieces, 256 // rows))

    def pooled_weights(h, g):
        cols = slice(h * HD, (h + 1) * HD)
        keys = jnp.concatenate([r[1, :, cols] for r in parts], axis=0)
        query = jnp.concatenate([r[0, :, cols] for r in parts[g : g + group]], axis=0)
        scores = lax.dot_general(
            query, keys, (((1,), (1,)), ((), ())), preferred_element_type=F32
        )
        peak = jnp.max(scores, axis=1, keepdims=True)
        exponent = jnp.exp2((scores - peak) * scale)
        share = 1.0 / (POOL * jnp.sum(exponent, axis=1, keepdims=True))
        return exponent * share

    @pl.when(me >= 0)
    def compute():
        rows_at = []
        for h in range(width // HD):
            for g in range(0, pieces, group):
                weights = pooled_weights(h, g)
                size = weights.shape[0]
                for c in range(pieces * rows // HD):
                    staged_ref[c, :size, :] = weights[:, c * HD : (c + 1) * HD]
                if not rows_at:
                    table.wait()
                    for k in ids:
                        token = (me ^ k) * kept
                        target = offsets[owner, token // block] // (kept * pieces)
                        start = (target ^ owner) * block + token % block
                        rows_at.append(pl.multiple_of(start, kept))
                for c in range(pieces * rows // HD):
                    total = sum(
                        staged_ref[c, pl.ds(r, size // POOL, stride=POOL), :]
                        for r in range(POOL)
                    ).astype(BF16)
                    for n in range(size // rows):
                        out[h, pl.ds(rows_at[g + n], kept), c * HD : (c + 1) * HD] = total[
                            n * kept : (n + 1) * kept, :
                        ]

    fetch.wait()


def score(offsets, w_proj, ids, parts, slots):
    rows, width = parts[0].shape[1:]
    keys = len(parts) * rows
    heads = width // HD
    group = max(1, min(len(parts), 256 // rows))
    return pl.pallas_call(
        functools.partial(
            score_body, ids=ids, slots=slots, scale=HD ** (-0.5) * math.log2(math.e)
        ),
        out_shape=[
            jax.ShapeDtypeStruct((heads, keys // POOL, keys), BF16),
            jax.ShapeDtypeStruct(w_proj.shape, BF16),
        ],
        in_specs=[hbm()] * 2 + [vmem()] * len(parts),
        out_specs=[vmem()] * 2,
        scratch_shapes=[
            pltpu.VMEM((keys // HD, group * rows, HD), F32),
            pltpu.SMEM(offsets.shape, jnp.int32),
            pltpu.SemaphoreType.DMA((2,)),
        ],
        compiler_params=limit(24),
        cost_estimate=pl.CostEstimate(
            flops=2 * keys * keys * width,
            bytes_accessed=0,
            transcendentals=keys * keys * heads,
        ),
        name="score",
    )(in_hbm(offsets), in_hbm(w_proj), *parts)


def mix_body(weight_ref, *refs, slots):
    parts, outs = refs[:-slots], refs[-slots:]
    block = outs[0].shape[0]
    for h in range(weight_ref.shape[0]):
        cols = slice(h * HD, (h + 1) * HD)
        values = jnp.concatenate([r[0, :, cols] for r in parts], axis=0)
        pooled = jnp.dot(weight_ref[h], values, preferred_element_type=F32).astype(BF16)
        for s in range(slots):
            outs[s][:, cols] = pooled[s * block : (s + 1) * block, :]


def mix(weights, parts, slots, block):
    width = parts[0].shape[2]
    return pl.pallas_call(
        functools.partial(mix_body, slots=slots),
        out_shape=[jax.ShapeDtypeStruct((block, width), BF16)] * slots,
        in_specs=[vmem()] * (1 + len(parts)),
        out_specs=[vmem()] * slots,
        compiler_params=limit(8),
        name="mix",
    )(weights, *parts)


def plan_body(offsets, counts, pick_ref, live_ref, *, slots):
    owner = lax.axis_index("img")
    rows = live_ref.shape[0]
    block = rows // slots
    slot_ids = lax.broadcasted_iota(jnp.int32, (slots, HD), 0)
    row_ids = lax.broadcasted_iota(jnp.int32, (block, HD), 0)
    for s in range(slots):
        source = owner ^ s

        def find(j, found):
            offset = offsets[source, j]
            here = offset // rows == owner
            return (
                jnp.where(here, (offset - owner * rows) // block, found[0]),
                jnp.where(here, counts[source] - j * block, found[1]),
            )

        slot, kept = lax.fori_loop(
            0, slots, find, (jnp.int32(0), jnp.int32(0)), unroll=slots <= 4
        )
        pick_ref[s] = (slot_ids == slot).astype(F32)
        start = pl.multiple_of(slot * block, block)
        live_ref[pl.ds(start, block), :] = (row_ids < kept).astype(F32)


def plan(offsets, counts, rows):
    slots = offsets.shape[0]
    return pl.pallas_call(
        functools.partial(plan_body, slots=slots),
        out_shape=[
            jax.ShapeDtypeStruct((slots, slots, HD), F32),
            jax.ShapeDtypeStruct((rows, HD), F32),
        ],
        in_specs=[smem()] * 2,
        out_specs=[vmem()] * 2,
        compiler_params=limit(2),
        name="plan",
    )(offsets, counts)


def join_body(pick_ref, *refs):
    blocks, out = refs[:-1], refs[-1]
    block, width = blocks[0].shape
    for c in range(0, width, HD):
        values = [r[:, c : c + HD].astype(F32) for r in blocks]
        for t in range(len(blocks)):
            total = sum(v * pick_ref[s, t : t + 1, :] for s, v in enumerate(values))
            out[t * block : (t + 1) * block, c : c + HD] = total.astype(BF16)


def join(pick, blocks):
    block, width = blocks[0].shape
    return pl.pallas_call(
        join_body,
        out_shape=jax.ShapeDtypeStruct((block * len(blocks), width), BF16),
        in_specs=[vmem()] * (1 + len(blocks)),
        out_specs=vmem(),
        compiler_params=limit(2),
        name="join",
    )(pick, *blocks)


def product(ids, parts, w_ref):
    me = lax.axis_index("seq")
    total = None
    width = parts[0].shape[1]
    for n, part in zip(ids, parts):
        start = pl.multiple_of((me ^ n) * width, HD)
        term = jnp.dot(part[...], w_ref[pl.ds(start, width), :], preferred_element_type=F32)
        total = term if total is None else total + term
    return total


def project_body(*refs, ids, carried):
    pieces = len(ids)
    parts, w_ref, out = refs[:pieces], refs[pieces], refs[-1]
    total = product(ids, parts, w_ref)
    if carried:
        total = total + refs[pieces + 1][...]
    out[...] = total


def project(ids, parts, w_proj, carry):
    rows, width = parts[0].shape
    carried = carry is not None
    return pl.pallas_call(
        functools.partial(project_body, ids=ids, carried=carried),
        out_shape=jax.ShapeDtypeStruct((rows, w_proj.shape[1]), F32),
        in_specs=[vmem()] * (len(parts) + 1 + carried),
        out_specs=vmem(),
        cost_estimate=pl.CostEstimate(
            flops=2 * rows * width * len(parts) * w_proj.shape[1],
            bytes_accessed=0,
            transcendentals=0,
        ),
        compiler_params=limit(14),
        name="project",
    )(*parts, w_proj, *([carry] if carried else []))


def hide_body(*refs, ids, carried):
    pieces = len(ids)
    parts, w_ref, text_ref, live_ref = refs[:pieces], *refs[pieces : pieces + 3]
    hidden_ref, square_ref = refs[-2:]
    total = product(ids, parts, w_ref)
    if carried:
        total = total + refs[pieces + 3][...]
    live = live_ref[...] > 0.5
    partial = None
    for c in range(0, hidden_ref.shape[1], HD):
        value = jnp.where(
            live, total[:, c : c + HD], text_ref[:, c : c + HD].astype(F32)
        )
        hidden_ref[:, c : c + HD] = value
        partial = value * value if partial is None else partial + value * value
    square_ref[...] = jnp.sum(partial.T, axis=0, keepdims=True)


def hide(ids, parts, w_proj, text, live, carry):
    rows, width = text.shape
    carried = carry is not None
    return pl.pallas_call(
        functools.partial(hide_body, ids=ids, carried=carried),
        out_shape=[
            jax.ShapeDtypeStruct((rows, width), F32),
            jax.ShapeDtypeStruct((1, rows), F32),
        ],
        in_specs=[vmem()] * (len(parts) + 3 + carried),
        out_specs=[vmem()] * 2,
        compiler_params=limit(18),
        name="hide",
    )(*parts, w_proj, text, live, *([carry] if carried else []))


def norm_body(*refs, features):
    hidden_ref, gain_ref, out = refs[0], refs[1], refs[-1]
    total = sum(r[...] for r in refs[2:-1])
    inverse = lax.rsqrt(total / features + EPSILON)
    rows, width = hidden_ref.shape
    column = jnp.broadcast_to(inverse, (128, rows)).T
    for c in range(0, width, 128):
        out[:, c : c + 128] = (
            hidden_ref[:, c : c + 128] * column * gain_ref[:, c : c + 128]
        ).astype(BF16)


def norm(hidden, gain, sums, features):
    return pl.pallas_call(
        functools.partial(norm_body, features=features),
        out_shape=jax.ShapeDtypeStruct(hidden.shape, BF16),
        in_specs=[vmem()] * (2 + len(sums)),
        out_specs=vmem(),
        compiler_params=limit(4),
        name="norm",
    )(hidden, gain, *sums)


def on_device(queries, keys, values, counts, offsets, text, w_proj, gain):
    members = lax.axis_size("seq")
    owners = lax.axis_size("img")
    block = queries.shape[1] // POOL * members // owners
    chips = members // 2

    def swap(x, axis, k):
        pairs = [(j, j ^ k) for j in range(lax.axis_size(axis))]
        return lax.ppermute(x, axis, pairs)

    order = seq_order(members)

    def exchange(tensors):
        sent = pack(tensors, members)
        return [sent[0]] + [swap(sent[k], "seq", k) for k in order[1:]]

    pairs = exchange([queries, keys])
    singles = exchange([values])
    weights, weight = score(offsets, w_proj, order, pairs, owners)
    outgoing = mix(weights, singles, owners, block)
    pick, live = plan(offsets, counts, text.shape[0])
    blocks = [outgoing[0]] + [None] * (owners - 1)
    for k in img_order(owners):
        blocks[k] = swap(outgoing[k], "img", k)
    visual = join(pick, blocks)
    near = {0: visual}
    for k in chip_order(chips):
        near[k] = swap(visual, "seq", 2 * k)
    far = {}
    for k, x in near.items():
        far[k] = swap(x, "seq", 1)
    carry = None
    steps = project_steps(chips)
    for n, ids in enumerate(steps):
        parts = [far[i // 2] if i % 2 else near[i // 2] for i in ids]
        if n < len(steps) - 1:
            carry = project(ids, parts, weight, carry)
    hidden, square = hide(ids, parts, weight, text, live, carry)
    square = square + swap(square, "seq", 1)
    sums = [square] + [swap(square, "seq", 2 * k + 1) for k in square_order(chips)]
    return norm(hidden, gain[None, :], sums, members * text.shape[1])


def seq_order(members):
    cross = sorted(range(2, members), key=lambda k: ((k // 2).bit_count(), k % 2, k))
    return (0, *cross, 1)


def img_order(owners):
    return sorted(range(1, owners), key=lambda k: (k == 1, k.bit_count(), k))


def chip_order(chips):
    return sorted(range(1, chips), key=lambda k: (k.bit_count(), -k))


def square_order(chips):
    return sorted(range(1, chips), key=lambda k: (k != 1, -k))


def project_steps(chips):
    order = chip_order(chips)
    early = [i for k in order[:-2] for i in (2 * k, 2 * k + 1)]
    late = [i for k in order[-2:-1] for i in (2 * k, 2 * k + 1)]
    steps = [[0, 1], early, late + [2 * order[-1]], [2 * order[-1] + 1]]
    return [tuple(ids) for ids in steps if ids]


def solution(mesh):
    in_specs = (
        P("img", "seq", None),
        P("img", "seq", None),
        P("img", "seq", None),
        P(),
        P(),
        P("img", "seq"),
        P(None, "seq"),
        P("seq"),
    )
    out_specs = P("img", "seq")
    return jax.shard_map(
        on_device, mesh=mesh, in_specs=in_specs, out_specs=out_specs, check_vma=False
    )
```
